32 devices in a mesh: row: 8 (over z, core), col: 4 (over y, x).
Axes of the slice: x: 2, y: 2, z: 4, core: 2. Of those that a mesh axis runs over, the one named last changes fastest.
Arguments:
- fine_residual: float32 [16, 3, 1572864], P(None, None, ('row', 'col')), may hold values from -6 to 6
- restriction: float32 [3, 3, 1572864], P(None, None, ('row', 'col')), may hold values from -1.25 to 1.25
- restriction_pattern: int32 [1572864], P(('row', 'col')), may hold values 0 or 1
- cell_aggregate: int32 [384, 512], P('row', 'col'), may hold values from 0 to 196607, as said below
- block_inverse: float32 [3, 3, 384, 512], P(None, None, 'row', 'col'), may hold values from -4 to 4, as said below
- off_blocks: float32 [4, 3, 3, 384, 512], P(None, None, None, 'row', 'col'), may hold values from -0.5 to 0.5
- operator_pattern: int32 [4, 384, 512], P(None, 'row', 'col'), may hold values 0 or 1
Outputs:
- coarse_solution: float32 [16, 3, 384, 512], P(None, None, 'row', 'col')
- fine_correction: float32 [16, 3, 1572864], P(None, None, ('row', 'col'))
The draws below stay inside these ranges and needn't reach their ends.
Inputs may be any that keep to these rules, and one draw needn't show every extreme that they name: `cell_aggregate`: every aggregate number 0 to 196607 stands in exactly one coarse cell. Aggregate g = f * 6144 + a lies in the tile numbered a mod 32, where the tile of rows i * 48 to (i + 1) * 48 - 1 and columns j * 128 to (j + 1) * 128 - 1 is numbered i * 4 + j. `block_inverse`: each 3x3 block is the inverse of a cell's diagonal block.
All inputs are finite; a program needn't handle non-finite values. No bound on the sum of `restriction_pattern` or of `operator_pattern` on one device may be relied on, other than what follows from the above.
Results may differ from the reference program's by a relative error of at most 0.00002.
Values sent between devices are 32-bit elements; how exact they have to be, the bound alone decides.
A program may use at most 128 MiB of HBM per device.

```python
import jax
import jax.numpy as jnp

NRHS = 16
CR = 48
CC = 128
FPA = 8
ITERS = 4
AGG_DEV = 6144
FINE = 1572864
NCR = 384
NCC = 512
N_ROW = 8
N_COL = 4


def draw_cell_aggregate(key, part):
    devices = N_ROW * N_COL

    def tile_cells(tile):
        order = jax.random.permutation(jax.random.fold_in(key, tile), AGG_DEV)
        owner = order % devices
        local = order // devices * devices + tile
        return (owner * AGG_DEV + local).astype(jnp.int32)
    tiles = jax.vmap(tile_cells)(jnp.arange(devices, dtype=jnp.int32))
    grid = tiles.reshape(N_ROW, N_COL, CR, CC).transpose(0, 2, 1, 3)
    return grid.reshape(N_ROW * CR, N_COL * CC)


def draw_block_inverse(key, part):
    scale_key = jax.random.fold_in(key, 11)
    noise_key = jax.random.fold_in(key, 12)
    scale = jnp.exp(jax.random.uniform(scale_key, (NCR, NCC), jnp.float32, jnp.log(0.5), jnp.log(2.0)))
    noise = 0.3 * jnp.clip(jax.random.normal(noise_key, (3, 3, NCR, NCC), jnp.float32), -2.5, 2.5)
    identity = jnp.eye(3, dtype=jnp.float32)[:, :, None, None]
    return (scale[None, None] * (identity + noise)).astype(jnp.float32)


def touch_ends(result, rng, low, high):
    shape = result.shape
    place = [jax.random.randint(jax.random.fold_in(rng, axis), (), 0, shape[axis]) for axis in range(len(shape))]
    result = result.at[tuple(place)].set(low)
    longest = shape.index(max(shape))
    place[longest] = (place[longest] + 1) % shape[longest]
    return result.at[tuple(place)].set(high)


def block_scale(rng, dims, split, smallest, high):
    def one(dim, parts):
        heights = jax.random.uniform(jax.random.fold_in(jax.random.fold_in(rng, 6), dim), (parts,), jnp.float32, smallest / len(split), high / len(split))
        return jnp.repeat(jnp.exp(heights), dims[dim] // parts).reshape((-1,) + (1,) * (len(dims) - dim - 1))

    level = one(*split[0])
    for cut in split[1:]:
        level = level * one(*cut)
    return level


def centred(stream_key, extent, width, bound, pieces=(), kind=jnp.bfloat16):
    drawn = width * jax.random.normal(stream_key, extent, jnp.float32)
    if pieces:
        drawn = drawn * block_scale(stream_key, extent, pieces, -0.22, 0.18)
    return jnp.clip(drawn, -bound, bound).astype(kind)


def setup_inputs(seed: int = 0) -> dict:
    key_list = jax.random.split(jax.random.key(seed), 8)
    return {
        "fine_residual": centred(key_list[0], (NRHS, 3, FINE), 1.0, 6.0, ((2, 32),), jnp.float32),
        "restriction": centred(key_list[1], (3, 3, FINE), (3 * FPA) ** -0.5, 1.25, ((2, 32),), jnp.float32),
        "restriction_pattern": touch_ends((jax.random.randint(key_list[2], (FINE,), 0, 4) < 3).astype(jnp.int32), jax.random.fold_in(key_list[2], 1), 0, 1),
        "cell_aggregate": draw_cell_aggregate(jax.random.fold_in(key_list[7], 71), 0),
        "block_inverse": draw_block_inverse(jax.random.fold_in(key_list[7], 71), 0),
        "off_blocks": centred(key_list[5], (4, 3, 3, NCR, NCC), 0.1, 0.5, ((3, 8), (4, 4)), jnp.float32),
        "operator_pattern": touch_ends((jax.random.randint(key_list[6], (4, NCR, NCC), 0, 4) < 3).astype(jnp.int32), jax.random.fold_in(key_list[6], 1), 0, 1),
    }


def apply_inverse(inverse, vector):
    total = inverse[:, 0][None] * vector[:, 0][:, None]
    for source in range(1, 3):
        total = total + inverse[:, source][None] * vector[:, source][:, None]
    return total


def neighbours(padded):
    height = padded.shape[-2] - 2
    breadth = padded.shape[-1] - 2
    return (padded[..., 0:height, 1:breadth + 1], padded[..., 2:height + 2, 1:breadth + 1],
            padded[..., 1:height + 1, 0:breadth], padded[..., 1:height + 1, 2:breadth + 2])


def sweep_once(padded, target_side, inverse, coupling):
    total = target_side
    for direction, shifted in enumerate(neighbours(padded)):
        for source in range(3):
            total = total - coupling[direction, :, source][None] * shifted[:, source][:, None]
    return apply_inverse(inverse, total)


def restrict_terms(residual, restriction, pattern):
    masked = residual * pattern.astype(jnp.float32)[None, None]
    total = restriction[:, 0][None] * masked[:, 0][:, None]
    for source in range(1, 3):
        total = total + restriction[:, source][None] * masked[:, source][:, None]
    loads = total.shape[0]
    return total.reshape(loads, 3, -1, FPA, AGG_DEV).sum(axis=3).reshape(loads, 3, -1)


def prolong_terms(values, restriction, pattern):
    loads = values.shape[0]
    slabs = values.shape[2] // AGG_DEV
    expanded = jnp.broadcast_to(values.reshape(loads, 3, slabs, 1, AGG_DEV), (loads, 3, slabs, FPA, AGG_DEV)).reshape(loads, 3, -1)
    total = restriction[0][None] * expanded[:, 0][:, None]
    for source in range(1, 3):
        total = total + restriction[source][None] * expanded[:, source][:, None]
    return total * pattern.astype(jnp.float32)[None, None]


def reference(fine_residual, restriction, restriction_pattern, cell_aggregate, block_inverse, off_blocks, operator_pattern):
    loads = fine_residual.shape[0]
    aggregate_rhs = restrict_terms(fine_residual, restriction, restriction_pattern)
    flat_cells = cell_aggregate.reshape(-1)
    coarse_rhs = jnp.take(aggregate_rhs, flat_cells, axis=2).reshape(loads, 3, NCR, NCC)
    coupling = off_blocks * operator_pattern.astype(jnp.float32)[:, None, None]
    iterate = apply_inverse(block_inverse, coarse_rhs)
    for sweep_index in range(ITERS - 1):
        padded = jnp.pad(iterate, ((0, 0), (0, 0), (1, 1), (1, 1)))
        iterate = sweep_once(padded, coarse_rhs, block_inverse, coupling)
    aggregate_solution = jnp.zeros_like(aggregate_rhs).at[:, :, flat_cells].set(iterate.reshape(loads, 3, -1))
    fine_correction = prolong_terms(aggregate_solution, restriction, restriction_pattern)
    return iterate, fine_correction
```

```python
import functools

import jax
import jax.numpy as jnp
from jax import lax
from jax.experimental import pallas as pl
from jax.experimental.pallas import tpu as pltpu
from jax.sharding import PartitionSpec as P

FPA = 8
ITERS = 4
AGG_DEV = 6144
LANES = 128
GROUP = 8
MESH = pl.DeviceIdType.MESH
VMEM_LIMIT = 56 * 1024 * 1024


def spec_vmem():
    return pl.BlockSpec(memory_space=pltpu.VMEM)


def restrict_kernel(devices, loads, *refs):
    residuals = refs[0:FPA]
    restrictions = refs[FPA : 2 * FPA]
    patterns = refs[2 * FPA : 3 * FPA]
    out_ref = refs[3 * FPA]
    stage = refs[3 * FPA + 1]
    group = pl.program_id(0)
    groups = AGG_DEV // (LANES * GROUP)
    parts = LANES // devices
    rows = 3 * groups * parts
    for block in range(GROUP):
        lanes = slice(block * LANES, (block + 1) * LANES)
        totals = [None, None, None]
        for p in range(FPA):
            present = patterns[p][block : block + 1, :].astype(jnp.float32)
            for j in range(3):
                masked = residuals[p][j, :, lanes] * present
                for i in range(3):
                    term = restrictions[p][i, j : j + 1, lanes] * masked
                    totals[i] = term if totals[i] is None else totals[i] + term
        for i in range(3):
            stage[i, block * loads : (block + 1) * loads, :] = totals[i]
    for i in range(3):
        turned = stage[i].T
        for part in range(parts):
            start = i * groups * parts + group * parts + part
            out_ref[pl.ds(start, devices, stride=rows), :] = turned[part * devices : (part + 1) * devices, :]


def restrict(residual, restriction, pattern, devices):
    loads = residual.shape[0]
    residual = residual.transpose(1, 0, 2)
    pattern = pattern.reshape(-1, LANES)
    width = LANES * GROUP
    groups = AGG_DEV // width
    rows = 3 * groups * (LANES // devices)
    res_specs = [pl.BlockSpec((3, loads, width), functools.partial(lambda p, g: (0, 0, p * groups + g), p)) for p in range(FPA)]
    rst_specs = [pl.BlockSpec((3, 3, width), functools.partial(lambda p, g: (0, 0, p * groups + g), p)) for p in range(FPA)]
    pat_specs = [pl.BlockSpec((GROUP, LANES), functools.partial(lambda p, g: (p * groups + g, 0), p)) for p in range(FPA)]
    return pl.pallas_call(
        functools.partial(restrict_kernel, devices, loads),
        grid=(groups,),
        in_specs=res_specs + rst_specs + pat_specs,
        out_specs=pl.BlockSpec((devices * rows, LANES), lambda g: (0, 0)),
        out_shape=jax.ShapeDtypeStruct((devices * rows, LANES), jnp.float32),
        scratch_shapes=[pltpu.VMEM((3, LANES, LANES), jnp.float32)],
        compiler_params=pltpu.CompilerParams(vmem_limit_bytes=VMEM_LIMIT),
        name="restrict",
    )(*([residual] * FPA + [restriction] * FPA + [pattern] * FPA))


def gather_kernel(devices, loads, slots_ref, chunk_ref, out_ref, table, staged):
    groups = AGG_DEV // (LANES * GROUP)
    piece = groups * (LANES // devices)
    lane = lax.broadcasted_iota(jnp.int32, (piece, LANES), 1)

    def unpack(f, carry):
        base = f * (3 * piece)
        parts = [chunk_ref[pl.ds(base + i * piece, piece), :] for i in range(3)]
        for block in range(GROUP):
            moved = []
            for i in range(3):
                shift = ((i - block) * loads) % LANES
                moved.append(pltpu.roll(parts[i], shift, 1) if shift else parts[i])
            row = jnp.where(lane < loads, moved[0], jnp.where(lane < 2 * loads, moved[1], moved[2]))
            table[pl.ds(f * (GROUP * piece) + block * piece, piece), :] = row
        return carry

    lax.fori_loop(0, devices, unpack, 0)
    height = out_ref.shape[0] // (3 * loads)

    def take(r, carry):
        for c in range(LANES):
            staged[pl.ds(c, 1), :] = table[pl.ds(slots_ref[r * LANES + c], 1), :]
        turned = staged[...].T
        out_ref[pl.ds(r, 3 * loads, stride=height), :] = turned[: 3 * loads, :]
        return carry

    lax.fori_loop(0, height, take, 0)


def gather(slots, chunks, devices, loads, height):
    return pl.pallas_call(
        functools.partial(gather_kernel, devices, loads),
        in_specs=[pl.BlockSpec(memory_space=pltpu.SMEM), spec_vmem()],
        out_specs=spec_vmem(),
        out_shape=jax.ShapeDtypeStruct((3 * loads * height, LANES), jnp.float32),
        scratch_shapes=[pltpu.VMEM((AGG_DEV, LANES), jnp.float32), pltpu.VMEM((LANES, LANES), jnp.float32)],
        compiler_params=pltpu.CompilerParams(vmem_limit_bytes=VMEM_LIMIT),
        name="gather_cells",
    )(slots, chunks)


def scatter_kernel(devices, loads, slots_ref, solution_ref, out_ref, table, staged):
    groups = AGG_DEV // (LANES * GROUP)
    piece = groups * (LANES // devices)
    height = solution_ref.shape[0] // (3 * loads)
    staged[...] = jnp.zeros_like(staged)

    def put(r, carry):
        staged[:, : 3 * loads] = solution_ref[pl.ds(r, 3 * loads, stride=height), :].T
        for c in range(LANES):
            table[pl.ds(slots_ref[r * LANES + c], 1), :] = staged[pl.ds(c, 1), :]
        return carry

    lax.fori_loop(0, height, put, 0)
    lane = lax.broadcasted_iota(jnp.int32, (piece, LANES), 1)

    def pack(f, carry):
        rows = [table[pl.ds(f * (GROUP * piece) + block * piece, piece), :] for block in range(GROUP)]
        for i in range(3):
            total = None
            for block in range(GROUP):
                shift = ((block - i) * loads) % LANES
                moved = pltpu.roll(rows[block], shift, 1) if shift else rows[block]
                total = moved if total is None else jnp.where(lane < block * loads, total, moved)
            out_ref[pl.ds(f * (3 * piece) + i * piece, piece), :] = total
        return carry

    lax.fori_loop(0, devices, pack, 0)


def scatter(slots, solution_planes, devices, loads):
    groups = AGG_DEV // (LANES * GROUP)
    piece = groups * (LANES // devices)
    return pl.pallas_call(
        functools.partial(scatter_kernel, devices, loads),
        in_specs=[pl.BlockSpec(memory_space=pltpu.SMEM), spec_vmem()],
        out_specs=spec_vmem(),
        out_shape=jax.ShapeDtypeStruct((devices * 3 * piece, LANES), jnp.float32),
        scratch_shapes=[pltpu.VMEM((AGG_DEV, LANES), jnp.float32), pltpu.VMEM((LANES, LANES), jnp.float32)],
        compiler_params=pltpu.CompilerParams(vmem_limit_bytes=VMEM_LIMIT),
        name="scatter_cells",
    )(slots, solution_planes)


def sweep_kernel(
    row_count,
    col_count,
    loads,
    rhs_ref,
    inverse_ref,
    blocks_ref,
    pattern_ref,
    out_ref,
    planes_ref,
    base,
    x,
    mixed,
    sent,
    halo,
    send_sem,
    recv_sem,
):
    height = inverse_ref.shape[2]
    planes = 3 * loads
    row = lax.axis_index("row")
    col = lax.axis_index("col")
    exists = (row > 0, row < row_count - 1, col > 0, col < col_count - 1)
    peers = (
        {"row": row - 1, "col": col},
        {"row": row + 1, "col": col},
        {"row": row, "col": col - 1},
        {"row": row, "col": col + 1},
    )
    barrier = pltpu.get_barrier_semaphore()
    halo[...] = jnp.zeros_like(halo)
    for d in range(4):

        @pl.when(exists[d])
        def _():
            pl.semaphore_signal(barrier, inc=1, device_id=peers[d], device_id_type=MESH)

    def first(q, carry):
        for i in range(3):
            total = inverse_ref[i, 0] * rhs_ref[q]
            total = total + inverse_ref[i, 1] * rhs_ref[loads + q]
            total = total + inverse_ref[i, 2] * rhs_ref[2 * loads + q]
            base[i * loads + q] = total
            x[0, i * loads + q, 8 : 8 + height, :] = total
        return carry

    lax.fori_loop(0, loads, first, 0)
    lane = lax.broadcasted_iota(jnp.int32, (height, LANES), 1)

    def pack(slot, step):
        sent[step, 0] = x[slot, :, 8, :]
        sent[step, 1] = x[slot, :, 7 + height, :]

        def columns(p, carry):
            left, right = carry
            plane = x[slot, p, 8 : 8 + height, :]
            left = jnp.where(lane == p, pltpu.roll(plane, p, 1), left)
            right = jnp.where(lane == p, pltpu.roll(plane, p + 1, 1), right)
            return left, right

        blank = jnp.zeros((height, LANES), jnp.float32)
        left, right = lax.fori_loop(0, planes, columns, (blank, blank), unroll=4)
        sent[step, 2, :height, :] = left
        sent[step, 3, :height, :] = right

    def copies(step, d):
        return pltpu.make_async_remote_copy(
            src_ref=sent.at[step, d],
            dst_ref=halo.at[step, d ^ 1],
            send_sem=send_sem.at[step, d],
            recv_sem=recv_sem.at[step, d ^ 1],
            device_id=peers[d],
            device_id_type=MESH,
        )

    def receives(step, d):
        return pltpu.make_async_remote_copy(
            src_ref=sent.at[step, d],
            dst_ref=halo.at[step, d],
            send_sem=send_sem.at[step, d],
            recv_sem=recv_sem.at[step, d],
            device_id=peers[d],
            device_id_type=MESH,
        )

    pack(0, 0)
    present = sum(e.astype(jnp.int32) for e in exists)
    pl.semaphore_wait(barrier, present)
    for step in range(ITERS - 1):
        old = step % 2
        for d in range(4):

            @pl.when(exists[d])
            def _():
                copies(step, d).start()

        if step == 0:

            def fold(d, carry):
                on = pattern_ref[d].astype(jnp.float32)
                for k in range(3):
                    column = [blocks_ref[d, j, k] * on for j in range(3)]
                    for i in range(3):
                        total = inverse_ref[i, 0] * column[0]
                        total = total + inverse_ref[i, 1] * column[1]
                        mixed[d, i, k] = total + inverse_ref[i, 2] * column[2]
                return carry

            lax.fori_loop(0, 4, fold, 0)
        for d in range(4):

            @pl.when(exists[d])
            def _():
                copies(step, d).wait_send()
                receives(step, d).wait_recv()

        x[old, :, 7, :] = halo[step, 0]
        x[old, :, 8 + height, :] = halo[step, 1]
        last = step == ITERS - 2

        def update(q, carry):
            totals = [base[i * loads + q] for i in range(3)]
            for k in range(3):
                p = k * loads + q
                plane = x[old, p, 8 : 8 + height, :]
                left = jnp.where(
                    lane == 0, pltpu.roll(halo[step, 2, :height, :], lax.rem(LANES - p, LANES), 1), pltpu.roll(plane, 1, 1)
                )
                right = jnp.where(
                    lane == LANES - 1,
                    pltpu.roll(halo[step, 3, :height, :], LANES - 1 - p, 1),
                    pltpu.roll(plane, LANES - 1, 1),
                )
                shifted = (x[old, p, 7 : 7 + height, :], x[old, p, 9 : 9 + height, :], left, right)
                for d in range(4):
                    for i in range(3):
                        totals[i] = totals[i] - mixed[d, i, k] * shifted[d]
            for i in range(3):
                if last:
                    out_ref[q, i] = totals[i]
                    planes_ref[i * loads + q] = totals[i]
                else:
                    x[1 - old, i * loads + q, 8 : 8 + height, :] = totals[i]
            return carry

        lax.fori_loop(0, loads, update, 0)
        if not last:
            pack(1 - old, step + 1)


def sweeps(rhs, inverse, blocks, pattern, row_count, col_count, loads):
    height = inverse.shape[2]
    planes = 3 * loads
    steps = ITERS - 1
    span = max(planes, height)
    return pl.pallas_call(
        functools.partial(sweep_kernel, row_count, col_count, loads),
        in_specs=[spec_vmem()] * 4,
        out_specs=(spec_vmem(), spec_vmem()),
        out_shape=(
            jax.ShapeDtypeStruct((loads, 3, height, LANES), jnp.float32),
            jax.ShapeDtypeStruct((planes, height, LANES), jnp.float32),
        ),
        scratch_shapes=[
            pltpu.VMEM((planes, height, LANES), jnp.float32),
            pltpu.VMEM((2, planes, height + 16, LANES), jnp.float32),
            pltpu.VMEM((4, 3, 3, height, LANES), jnp.float32),
            pltpu.VMEM((steps, 4, span, LANES), jnp.float32),
            pltpu.VMEM((steps, 4, span, LANES), jnp.float32),
            pltpu.SemaphoreType.DMA((steps, 4)),
            pltpu.SemaphoreType.DMA((steps, 4)),
        ],
        compiler_params=pltpu.CompilerParams(
            vmem_limit_bytes=VMEM_LIMIT, collective_id=0, has_side_effects=True
        ),
        name="sweeps",
    )(rhs.reshape(planes, height, LANES), inverse, blocks, pattern)


def prolong_kernel(devices, loads, chunk_ref, restriction_ref, pattern_ref, out_ref, values):
    groups = AGG_DEV // (LANES * GROUP)
    parts = LANES // devices
    rows = 3 * groups * parts

    @pl.when(pl.program_id(0) == 0)
    def _():
        for i in range(3):
            for group in range(groups):
                start = i * groups * parts + group * parts
                pieces = [chunk_ref[pl.ds(start + part, devices, stride=rows), :] for part in range(parts)]
                values[i, group] = jnp.concatenate(pieces, axis=0).T if parts > 1 else pieces[0].T

    for group in range(groups):
        for block in range(GROUP):
            b = group * GROUP + block
            lanes = slice(b * LANES, (b + 1) * LANES)
            present = pattern_ref[b : b + 1, :].astype(jnp.float32)
            terms = [values[i, group, block * loads : (block + 1) * loads, :] * present for i in range(3)]
            for j in range(3):
                total = restriction_ref[0, j : j + 1, lanes] * terms[0]
                total = total + restriction_ref[1, j : j + 1, lanes] * terms[1]
                out_ref[j, :, lanes] = total + restriction_ref[2, j : j + 1, lanes] * terms[2]


def prolong(chunks, restriction, pattern, devices, loads):
    pattern = pattern.reshape(-1, LANES)
    blocks = AGG_DEV // LANES
    groups = blocks // GROUP
    out = pl.pallas_call(
        functools.partial(prolong_kernel, devices, loads),
        grid=(FPA,),
        in_specs=[
            pl.BlockSpec(chunks.shape, lambda p: (0, 0)),
            pl.BlockSpec((3, 3, AGG_DEV), lambda p: (0, 0, p)),
            pl.BlockSpec((blocks, LANES), lambda p: (p, 0)),
        ],
        out_specs=pl.BlockSpec((3, loads, AGG_DEV), lambda p: (0, 0, p)),
        out_shape=jax.ShapeDtypeStruct((3, loads, restriction.shape[2]), jnp.float32),
        scratch_shapes=[pltpu.VMEM((3, groups, GROUP * loads, LANES), jnp.float32)],
        compiler_params=pltpu.CompilerParams(vmem_limit_bytes=VMEM_LIMIT),
        name="prolong",
    )(chunks, restriction, pattern)
    return out.transpose(1, 0, 2)


def exchange(chunks, devices):
    parts = chunks.reshape(devices, -1, LANES)
    parts = lax.all_to_all(parts, ("row", "col"), split_axis=0, concat_axis=0, tiled=True)
    return parts.reshape(-1, LANES)


def body(
    fine_residual,
    restriction,
    restriction_pattern,
    cell_aggregate,
    block_inverse,
    off_blocks,
    operator_pattern,
):
    loads = fine_residual.shape[0]
    row_count = lax.axis_size("row")
    col_count = lax.axis_size("col")
    devices = row_count * col_count
    height = cell_aggregate.shape[0]
    parts = LANES // devices
    piece = AGG_DEV // (LANES * GROUP) * parts
    owner = cell_aggregate // AGG_DEV
    order = cell_aggregate % AGG_DEV // devices
    cell_block = order // parts
    slots = (
        owner * (GROUP * piece)
        + cell_block % GROUP * piece
        + cell_block // GROUP * parts
        + order % parts
    ).reshape(-1)
    outgoing = restrict(fine_residual, restriction, restriction_pattern, devices)
    received = exchange(outgoing, devices)
    rhs = gather(slots, received, devices, loads, height)
    iterate, planes = sweeps(rhs, block_inverse, off_blocks, operator_pattern, row_count, col_count, loads)
    returning = scatter(slots, planes.reshape(-1, LANES), devices, loads)
    arrived = exchange(returning, devices)
    fine_correction = prolong(arrived, restriction, restriction_pattern, devices, loads)
    return (iterate, fine_correction)


def solution(mesh):
    in_specs = (
        P(None, None, ("row", "col")),
        P(None, None, ("row", "col")),
        P(("row", "col")),
        P("row", "col"),
        P(None, None, "row", "col"),
        P(None, None, None, "row", "col"),
        P(None, "row", "col"),
    )
    out_specs = (P(None, None, "row", "col"), P(None, None, ("row", "col")))
    return jax.shard_map(body, mesh=mesh, in_specs=in_specs, out_specs=out_specs, check_vma=False)
```

```python
import functools

import jax
import jax.numpy as jnp
from jax import lax
from jax.experimental import pallas as pl
from jax.experimental.pallas import tpu as pltpu
from jax.sharding import PartitionSpec as P

FPA = 8
ITERS = 4
AGG_DEV = 6144
LANES = 128
GROUP = 8
PAIR = 2
MESH = pl.DeviceIdType.MESH
VMEM_LIMIT = 56 * 1024 * 1024


def spec_vmem():
    return pl.BlockSpec(memory_space=pltpu.VMEM)


def peer_of(me, index, devices, col_count):
    peer = lax.rem(me + 13 * index, devices)
    return peer, {"row": peer // col_count, "col": lax.rem(peer, col_count)}


def greet(devices, col_count, me):
    barrier = pltpu.get_barrier_semaphore()

    def signal(index, carry):
        _, where = peer_of(me, index, devices, col_count)
        pl.semaphore_signal(barrier, inc=1, device_id=where, device_id_type=MESH)
        return carry

    lax.fori_loop(1, devices, signal, 0)
    return barrier


def restrict_kernel(devices, col_count, loads, *refs):
    residuals = refs[0:FPA]
    restrictions = refs[FPA : 2 * FPA]
    patterns = refs[2 * FPA : 3 * FPA]
    out_ref, stage, sent, send_sem, recv_sem, own_sem = refs[3 * FPA :]
    pair = pl.program_id(0)
    pairs = pl.num_programs(0)
    parts = LANES // devices
    me = lax.axis_index("row") * col_count + lax.axis_index("col")
    barrier = pltpu.get_barrier_semaphore()

    @pl.when(pair == 0)
    def _():
        greet(devices, col_count, me)

    for half in range(PAIR):
        for block in range(GROUP):
            start = (half * GROUP + block) * LANES
            lanes = slice(start, start + LANES)
            totals = [None, None, None]
            for p in range(FPA):
                present = patterns[p][0, half * GROUP + block : half * GROUP + block + 1, :].astype(jnp.float32)
                for j in range(3):
                    masked = residuals[p][j, :, lanes] * present
                    for i in range(3):
                        term = restrictions[p][i, j : j + 1, lanes] * masked
                        totals[i] = term if totals[i] is None else totals[i] + term
            for i in range(3):
                stage[i, block * loads : (block + 1) * loads, :] = totals[i]
        for i in range(3):
            turned = stage[i].T
            for part in range(parts):
                sent[pair, :, (i * PAIR + half) * parts + part, :] = turned[part * devices : (part + 1) * devices, :]

    @pl.when(pair == 0)
    def _():
        pl.semaphore_wait(barrier, devices - 1)

    def send(index, carry):
        peer, where = peer_of(me, index, devices, col_count)
        pltpu.make_async_remote_copy(
            src_ref=sent.at[pair, peer],
            dst_ref=out_ref.at[pair, me],
            send_sem=send_sem,
            recv_sem=recv_sem,
            device_id=where,
            device_id_type=MESH,
        ).start()
        return carry

    lax.fori_loop(1, devices, send, 0)

    @pl.when(pair == pairs - 1)
    def _():
        own = pltpu.make_async_copy(sent.at[:, me], out_ref.at[:, me], own_sem)
        own.start()
        own.wait()
        _, where = peer_of(me, 1, devices, col_count)
        every = pltpu.make_async_remote_copy(
            src_ref=sent.at[:, pl.ds(0, devices - 1)],
            dst_ref=out_ref.at[:, pl.ds(0, devices - 1)],
            send_sem=send_sem,
            recv_sem=recv_sem,
            device_id=where,
            device_id_type=MESH,
        )
        every.wait_send()
        every.wait_recv()


def restrict(residual, restriction, pattern, devices, col_count):
    loads = residual.shape[0]
    residual = residual.transpose(1, 0, 2)
    width = LANES * GROUP * PAIR
    pairs = AGG_DEV // width
    pattern = pattern.reshape(-1, GROUP * PAIR, LANES)
    rows = 3 * PAIR * (LANES // devices)
    res_specs = [pl.BlockSpec((3, loads, width), functools.partial(lambda p, g: (0, 0, p * pairs + g), p)) for p in range(FPA)]
    rst_specs = [pl.BlockSpec((3, 3, width), functools.partial(lambda p, g: (0, 0, p * pairs + g), p)) for p in range(FPA)]
    pat_specs = [pl.BlockSpec((1, GROUP * PAIR, LANES), functools.partial(lambda p, g: (p * pairs + g, 0, 0), p)) for p in range(FPA)]
    return pl.pallas_call(
        functools.partial(restrict_kernel, devices, col_count, loads),
        grid=(pairs,),
        in_specs=res_specs + rst_specs + pat_specs,
        out_specs=pl.BlockSpec(memory_space=pl.ANY),
        out_shape=jax.ShapeDtypeStruct((pairs, devices, rows, LANES), jnp.float32),
        scratch_shapes=[
            pltpu.VMEM((3, LANES, LANES), jnp.float32),
            pltpu.VMEM((pairs, devices, rows, LANES), jnp.float32),
            pltpu.SemaphoreType.DMA,
            pltpu.SemaphoreType.DMA,
            pltpu.SemaphoreType.DMA,
        ],
        compiler_params=pltpu.CompilerParams(
            vmem_limit_bytes=VMEM_LIMIT,
            collective_id=1,
            has_side_effects=True,
            dimension_semantics=("arbitrary",),
        ),
        name="restrict_send",
    )(*([residual] * FPA + [restriction] * FPA + [pattern] * FPA))


def gather_kernel(devices, loads, slots_ref, chunk_ref, out_ref, table, ordered):
    pairs = chunk_ref.shape[0]
    few = PAIR * (LANES // devices)
    piece = pairs * few
    lane = lax.broadcasted_iota(jnp.int32, (few, LANES), 1)

    def unpack(f, carry):
        for pair in range(pairs):
            parts = [chunk_ref[pair, f, i * few : (i + 1) * few, :] for i in range(3)]
            for block in range(GROUP):
                moved = []
                for i in range(3):
                    shift = ((i - block) * loads) % LANES
                    moved.append(pltpu.roll(parts[i], shift, 1) if shift else parts[i])
                row = jnp.where(lane < loads, moved[0], jnp.where(lane < 2 * loads, moved[1], moved[2]))
                table[pl.ds(f * (GROUP * piece) + block * piece + pair * few, few), :] = row
        return carry

    lax.fori_loop(0, devices, unpack, 0, unroll=2)
    height = out_ref.shape[0] // (3 * loads)

    def take(r, carry):
        for c in range(LANES):
            ordered[pl.ds(r * LANES + c, 1), :] = table[pl.ds(slots_ref[r * LANES + c], 1), :]
        return carry

    lax.fori_loop(0, height, take, 0)

    def turn(r, carry):
        turned = ordered[pl.ds(pl.multiple_of(r * LANES, LANES), LANES), :].T
        out_ref[pl.ds(r, 3 * loads, stride=height), :] = turned[: 3 * loads, :]
        return carry

    lax.fori_loop(0, height, turn, 0, unroll=4)


def gather(slots, chunks, devices, loads, height):
    return pl.pallas_call(
        functools.partial(gather_kernel, devices, loads),
        in_specs=[pl.BlockSpec(memory_space=pltpu.SMEM), spec_vmem()],
        out_specs=spec_vmem(),
        out_shape=jax.ShapeDtypeStruct((3 * loads * height, LANES), jnp.float32),
        scratch_shapes=[pltpu.VMEM((AGG_DEV, LANES), jnp.float32), pltpu.VMEM((height * LANES, LANES), jnp.float32)],
        compiler_params=pltpu.CompilerParams(vmem_limit_bytes=VMEM_LIMIT),
        name="gather_cells",
    )(slots, chunks)


def scatter_kernel(loads, slots_ref, solution_ref, table, ordered):
    height = solution_ref.shape[0] // (3 * loads)

    def turn(r, carry):
        plane = solution_ref[pl.ds(r, 3 * loads, stride=height), :]
        ordered[pl.ds(pl.multiple_of(r * LANES, LANES), LANES), : 3 * loads] = plane.T
        return carry

    lax.fori_loop(0, height, turn, 0, unroll=4)

    def put(r, carry):
        for c in range(LANES):
            table[pl.ds(slots_ref[r * LANES + c], 1), :] = ordered[pl.ds(r * LANES + c, 1), :]
        return carry

    lax.fori_loop(0, height, put, 0)


def scatter(slots, solution_planes, loads):
    height = solution_planes.shape[0] // (3 * loads)
    return pl.pallas_call(
        functools.partial(scatter_kernel, loads),
        in_specs=[pl.BlockSpec(memory_space=pltpu.SMEM), spec_vmem()],
        out_specs=spec_vmem(),
        out_shape=jax.ShapeDtypeStruct((AGG_DEV, LANES), jnp.float32),
        scratch_shapes=[pltpu.VMEM((height * LANES, LANES), jnp.float32)],
        compiler_params=pltpu.CompilerParams(vmem_limit_bytes=VMEM_LIMIT),
        name="scatter_cells",
    )(slots, solution_planes)


def pack_kernel(devices, col_count, loads, table, out_ref, sent, send_sem, recv_sem, own_sem):
    piece = AGG_DEV // (GROUP * devices)
    me = lax.axis_index("row") * col_count + lax.axis_index("col")
    barrier = greet(devices, col_count, me)
    lane = lax.broadcasted_iota(jnp.int32, (piece, LANES), 1)

    def pack(f):
        rows = [table[pl.ds(f * (GROUP * piece) + block * piece, piece), :] for block in range(GROUP)]
        for i in range(3):
            total = None
            for block in range(GROUP):
                shift = ((block - i) * loads) % LANES
                moved = pltpu.roll(rows[block], shift, 1) if shift else rows[block]
                total = moved if total is None else jnp.where(lane < block * loads, total, moved)
            sent[f, i * piece : (i + 1) * piece, :] = total

    pack(me)
    own = pltpu.make_async_copy(sent.at[me], out_ref.at[me], own_sem)
    own.start()
    pl.semaphore_wait(barrier, devices - 1)

    def send(index, carry):
        peer, where = peer_of(me, index, devices, col_count)
        pack(peer)
        pltpu.make_async_remote_copy(
            src_ref=sent.at[peer],
            dst_ref=out_ref.at[me],
            send_sem=send_sem,
            recv_sem=recv_sem,
            device_id=where,
            device_id_type=MESH,
        ).start()
        return carry

    lax.fori_loop(1, devices, send, 0)
    own.wait()
    _, where = peer_of(me, 1, devices, col_count)
    every = pltpu.make_async_remote_copy(
        src_ref=sent.at[pl.ds(0, devices - 1)],
        dst_ref=out_ref.at[pl.ds(0, devices - 1)],
        send_sem=send_sem,
        recv_sem=recv_sem,
        device_id=where,
        device_id_type=MESH,
    )
    every.wait_send()
    every.wait_recv()


def pack_send(table, devices, col_count, loads):
    piece = AGG_DEV // (GROUP * devices)
    return pl.pallas_call(
        functools.partial(pack_kernel, devices, col_count, loads),
        in_specs=[spec_vmem()],
        out_specs=pl.BlockSpec(memory_space=pl.ANY),
        out_shape=jax.ShapeDtypeStruct((devices, 3 * piece, LANES), jnp.float32),
        scratch_shapes=[
            pltpu.VMEM((devices, 3 * piece, LANES), jnp.float32),
            pltpu.SemaphoreType.DMA,
            pltpu.SemaphoreType.DMA,
            pltpu.SemaphoreType.DMA,
        ],
        compiler_params=pltpu.CompilerParams(vmem_limit_bytes=VMEM_LIMIT, collective_id=2, has_side_effects=True),
        name="pack_send",
    )(table)


def sweep_kernel(
    row_count,
    col_count,
    loads,
    rhs_ref,
    inverse_ref,
    blocks_ref,
    pattern_ref,
    out_ref,
    planes_ref,
    base,
    x,
    mixed,
    sent,
    halo,
    send_sem,
    recv_sem,
):
    height = inverse_ref.shape[2]
    planes = 3 * loads
    row = lax.axis_index("row")
    col = lax.axis_index("col")
    exists = (row > 0, row < row_count - 1, col > 0, col < col_count - 1)
    peers = (
        {"row": row - 1, "col": col},
        {"row": row + 1, "col": col},
        {"row": row, "col": col - 1},
        {"row": row, "col": col + 1},
    )
    barrier = pltpu.get_barrier_semaphore()
    halo[...] = jnp.zeros_like(halo)
    for d in range(4):

        @pl.when(exists[d])
        def _():
            pl.semaphore_signal(barrier, inc=1, device_id=peers[d], device_id_type=MESH)

    def first(q, carry):
        for i in range(3):
            total = inverse_ref[i, 0] * rhs_ref[q]
            total = total + inverse_ref[i, 1] * rhs_ref[loads + q]
            total = total + inverse_ref[i, 2] * rhs_ref[2 * loads + q]
            base[i * loads + q] = total
            x[0, i * loads + q, 8 : 8 + height, :] = total
        return carry

    lax.fori_loop(0, loads, first, 0)
    lane = lax.broadcasted_iota(jnp.int32, (height, LANES), 1)

    def pack(slot, step):
        sent[step, 0] = x[slot, :, 8, :]
        sent[step, 1] = x[slot, :, 7 + height, :]

        def columns(p, carry):
            left, right = carry
            plane = x[slot, p, 8 : 8 + height, :]
            left = jnp.where(lane == p, pltpu.roll(plane, p, 1), left)
            right = jnp.where(lane == p, pltpu.roll(plane, p + 1, 1), right)
            return left, right

        blank = jnp.zeros((height, LANES), jnp.float32)
        left, right = lax.fori_loop(0, planes, columns, (blank, blank), unroll=4)
        sent[step, 2, :height, :] = left
        sent[step, 3, :height, :] = right

    def copies(step, d):
        return pltpu.make_async_remote_copy(
            src_ref=sent.at[step, d],
            dst_ref=halo.at[step, d ^ 1],
            send_sem=send_sem.at[step, d],
            recv_sem=recv_sem.at[step, d ^ 1],
            device_id=peers[d],
            device_id_type=MESH,
        )

    def receives(step, d):
        return pltpu.make_async_remote_copy(
            src_ref=sent.at[step, d],
            dst_ref=halo.at[step, d],
            send_sem=send_sem.at[step, d],
            recv_sem=recv_sem.at[step, d],
            device_id=peers[d],
            device_id_type=MESH,
        )

    pack(0, 0)
    present = sum(e.astype(jnp.int32) for e in exists)
    pl.semaphore_wait(barrier, present)
    for step in range(ITERS - 1):
        old = step % 2
        for d in range(4):

            @pl.when(exists[d])
            def _():
                copies(step, d).start()

        if step == 0:

            def fold(d, carry):
                on = pattern_ref[d].astype(jnp.float32)
                for k in range(3):
                    column = [blocks_ref[d, j, k] * on for j in range(3)]
                    for i in range(3):
                        total = inverse_ref[i, 0] * column[0]
                        total = total + inverse_ref[i, 1] * column[1]
                        mixed[d, i, k] = total + inverse_ref[i, 2] * column[2]
                return carry

            lax.fori_loop(0, 4, fold, 0)
        for d in range(4):

            @pl.when(exists[d])
            def _():
                copies(step, d).wait_send()
                receives(step, d).wait_recv()

        x[old, :, 7, :] = halo[step, 0]
        x[old, :, 8 + height, :] = halo[step, 1]
        last = step == ITERS - 2

        def update(q, carry):
            totals = [base[i * loads + q] for i in range(3)]
            for k in range(3):
                p = k * loads + q
                plane = x[old, p, 8 : 8 + height, :]
                left = jnp.where(
                    lane == 0, pltpu.roll(halo[step, 2, :height, :], lax.rem(LANES - p, LANES), 1), pltpu.roll(plane, 1, 1)
                )
                right = jnp.where(
                    lane == LANES - 1,
                    pltpu.roll(halo[step, 3, :height, :], LANES - 1 - p, 1),
                    pltpu.roll(plane, LANES - 1, 1),
                )
                shifted = (x[old, p, 7 : 7 + height, :], x[old, p, 9 : 9 + height, :], left, right)
                for d in range(4):
                    for i in range(3):
                        totals[i] = totals[i] - mixed[d, i, k] * shifted[d]
            for i in range(3):
                if last:
                    out_ref[q, i] = totals[i]
                    planes_ref[i * loads + q] = totals[i]
                else:
                    x[1 - old, i * loads + q, 8 : 8 + height, :] = totals[i]
            return carry

        lax.fori_loop(0, loads, update, 0)
        if not last:
            pack(1 - old, step + 1)


def sweeps(rhs, inverse, blocks, pattern, row_count, col_count, loads):
    height = inverse.shape[2]
    planes = 3 * loads
    steps = ITERS - 1
    span = max(planes, height)
    return pl.pallas_call(
        functools.partial(sweep_kernel, row_count, col_count, loads),
        in_specs=[spec_vmem()] * 4,
        out_specs=(spec_vmem(), spec_vmem()),
        out_shape=(
            jax.ShapeDtypeStruct((loads, 3, height, LANES), jnp.float32),
            jax.ShapeDtypeStruct((planes, height, LANES), jnp.float32),
        ),
        scratch_shapes=[
            pltpu.VMEM((planes, height, LANES), jnp.float32),
            pltpu.VMEM((2, planes, height + 16, LANES), jnp.float32),
            pltpu.VMEM((4, 3, 3, height, LANES), jnp.float32),
            pltpu.VMEM((steps, 4, span, LANES), jnp.float32),
            pltpu.VMEM((steps, 4, span, LANES), jnp.float32),
            pltpu.SemaphoreType.DMA((steps, 4)),
            pltpu.SemaphoreType.DMA((steps, 4)),
        ],
        compiler_params=pltpu.CompilerParams(
            vmem_limit_bytes=VMEM_LIMIT, collective_id=0, has_side_effects=True
        ),
        name="sweeps",
    )(rhs.reshape(planes, height, LANES), inverse, blocks, pattern)


def prolong_kernel(devices, loads, chunk_ref, restriction_ref, pattern_ref, out_ref, values):
    groups = AGG_DEV // (LANES * GROUP)
    parts = LANES // devices
    rows = 3 * groups * parts

    @pl.when(pl.program_id(0) == 0)
    def _():
        for i in range(3):
            for group in range(groups):
                start = i * groups * parts + group * parts
                pieces = [chunk_ref[pl.ds(start + part, devices, stride=rows), :] for part in range(parts)]
                values[i, group] = jnp.concatenate(pieces, axis=0).T if parts > 1 else pieces[0].T

    for group in range(groups):
        for block in range(GROUP):
            b = group * GROUP + block
            lanes = slice(b * LANES, (b + 1) * LANES)
            present = pattern_ref[b : b + 1, :].astype(jnp.float32)
            terms = [values[i, group, block * loads : (block + 1) * loads, :] * present for i in range(3)]
            for j in range(3):
                total = restriction_ref[0, j : j + 1, lanes] * terms[0]
                total = total + restriction_ref[1, j : j + 1, lanes] * terms[1]
                out_ref[j, :, lanes] = total + restriction_ref[2, j : j + 1, lanes] * terms[2]


def prolong(chunks, restriction, pattern, devices, loads):
    pattern = pattern.reshape(-1, LANES)
    blocks = AGG_DEV // LANES
    groups = blocks // GROUP
    out = pl.pallas_call(
        functools.partial(prolong_kernel, devices, loads),
        grid=(FPA,),
        in_specs=[
            pl.BlockSpec(chunks.shape, lambda p: (0, 0)),
            pl.BlockSpec((3, 3, AGG_DEV), lambda p: (0, 0, p)),
            pl.BlockSpec((blocks, LANES), lambda p: (p, 0)),
        ],
        out_specs=pl.BlockSpec((3, loads, AGG_DEV), lambda p: (0, 0, p)),
        out_shape=jax.ShapeDtypeStruct((3, loads, restriction.shape[2]), jnp.float32),
        scratch_shapes=[pltpu.VMEM((3, groups, GROUP * loads, LANES), jnp.float32)],
        compiler_params=pltpu.CompilerParams(vmem_limit_bytes=VMEM_LIMIT),
        name="prolong",
    )(chunks, restriction, pattern)
    return out.transpose(1, 0, 2)


def body(
    fine_residual,
    restriction,
    restriction_pattern,
    cell_aggregate,
    block_inverse,
    off_blocks,
    operator_pattern,
):
    loads = fine_residual.shape[0]
    row_count = lax.axis_size("row")
    col_count = lax.axis_size("col")
    devices = row_count * col_count
    height = cell_aggregate.shape[0]
    parts = LANES // devices
    piece = AGG_DEV // (LANES * GROUP) * parts
    owner = cell_aggregate // AGG_DEV
    order = cell_aggregate % AGG_DEV // devices
    cell_block = order // parts
    slots = (
        owner * (GROUP * piece)
        + cell_block % GROUP * piece
        + cell_block // GROUP * parts
        + order % parts
    ).reshape(-1)
    received = restrict(fine_residual, restriction, restriction_pattern, devices, col_count)
    rhs = gather(slots, received, devices, loads, height)
    iterate, planes = sweeps(rhs, block_inverse, off_blocks, operator_pattern, row_count, col_count, loads)
    table = scatter(slots, planes.reshape(-1, LANES), loads)
    arrived = pack_send(table, devices, col_count, loads).reshape(-1, LANES)
    fine_correction = prolong(arrived, restriction, restriction_pattern, devices, loads)
    return (iterate, fine_correction)


def solution(mesh):
    in_specs = (
        P(None, None, ("row", "col")),
        P(None, None, ("row", "col")),
        P(("row", "col")),
        P("row", "col"),
        P(None, None, "row", "col"),
        P(None, None, None, "row", "col"),
        P(None, "row", "col"),
    )
    out_specs = (P(None, None, "row", "col"), P(None, None, ("row", "col")))
    return jax.shard_map(body, mesh=mesh, in_specs=in_specs, out_specs=out_specs, check_vma=False)
```

```python
import functools

import jax
import jax.numpy as jnp
from jax import lax
from jax.experimental import pallas as pl
from jax.experimental.pallas import tpu as pltpu
from jax.sharding import PartitionSpec as P

FPA = 8
ITERS = 4
AGG_DEV = 6144
LANES = 128
GROUP = 8
PAIR = 2
HALVES = 2
MESH = pl.DeviceIdType.MESH
VMEM_LIMIT = 56 * 1024 * 1024


def spec_vmem():
    return pl.BlockSpec(memory_space=pltpu.VMEM)


def peer_of(me, index, devices, col_count):
    peer = lax.rem(me + 13 * index, devices)
    return peer, {"row": peer // col_count, "col": lax.rem(peer, col_count)}


def greet(devices, col_count, me):
    barrier = pltpu.get_barrier_semaphore()

    def signal(index, carry):
        _, where = peer_of(me, index, devices, col_count)
        pl.semaphore_signal(barrier, inc=1, device_id=where, device_id_type=MESH)
        return carry

    lax.fori_loop(1, devices, signal, 0)
    return barrier


def restrict_kernel(devices, col_count, loads, *refs):
    residuals = refs[0:FPA]
    restrictions = refs[FPA : 2 * FPA]
    patterns = refs[2 * FPA : 3 * FPA]
    out_ref, stage, sent, send_sem, recv_sem, own_sem = refs[3 * FPA :]
    pair = pl.program_id(0)
    pairs = pl.num_programs(0)
    parts = LANES // devices
    me = lax.axis_index("row") * col_count + lax.axis_index("col")
    barrier = pltpu.get_barrier_semaphore()

    @pl.when(pair == 0)
    def _():
        greet(devices, col_count, me)

    for half in range(PAIR):
        for block in range(GROUP):
            start = (half * GROUP + block) * LANES
            lanes = slice(start, start + LANES)
            totals = [None, None, None]
            for p in range(FPA):
                present = patterns[p][0, half * GROUP + block : half * GROUP + block + 1, :].astype(jnp.float32)
                for j in range(3):
                    masked = residuals[p][j, :, lanes] * present
                    for i in range(3):
                        term = restrictions[p][i, j : j + 1, lanes] * masked
                        totals[i] = term if totals[i] is None else totals[i] + term
            for i in range(3):
                stage[i, block * loads : (block + 1) * loads, :] = totals[i]
        for i in range(3):
            turned = stage[i].T
            for part in range(parts):
                sent[pair, :, (i * PAIR + half) * parts + part, :] = turned[part * devices : (part + 1) * devices, :]

    @pl.when(pair == 0)
    def _():
        pl.semaphore_wait(barrier, devices - 1)

    def send(index, carry):
        peer, where = peer_of(me, index, devices, col_count)
        pltpu.make_async_remote_copy(
            src_ref=sent.at[pair, peer],
            dst_ref=out_ref.at[pair, me],
            send_sem=send_sem,
            recv_sem=recv_sem,
            device_id=where,
            device_id_type=MESH,
        ).start()
        return carry

    lax.fori_loop(1, devices, send, 0)

    @pl.when(pair == pairs - 1)
    def _():
        own = pltpu.make_async_copy(sent.at[:, me], out_ref.at[:, me], own_sem)
        own.start()
        own.wait()
        _, where = peer_of(me, 1, devices, col_count)
        every = pltpu.make_async_remote_copy(
            src_ref=sent.at[:, pl.ds(0, devices - 1)],
            dst_ref=out_ref.at[:, pl.ds(0, devices - 1)],
            send_sem=send_sem,
            recv_sem=recv_sem,
            device_id=where,
            device_id_type=MESH,
        )
        every.wait_send()
        every.wait_recv()


def restrict(residual, restriction, pattern, devices, col_count):
    loads = residual.shape[0]
    residual = residual.transpose(1, 0, 2)
    width = LANES * GROUP * PAIR
    pairs = AGG_DEV // width
    pattern = pattern.reshape(-1, GROUP * PAIR, LANES)
    rows = 3 * PAIR * (LANES // devices)
    res_specs = [pl.BlockSpec((3, loads, width), functools.partial(lambda p, g: (0, 0, p * pairs + g), p)) for p in range(FPA)]
    rst_specs = [pl.BlockSpec((3, 3, width), functools.partial(lambda p, g: (0, 0, p * pairs + g), p)) for p in range(FPA)]
    pat_specs = [pl.BlockSpec((1, GROUP * PAIR, LANES), functools.partial(lambda p, g: (p * pairs + g, 0, 0), p)) for p in range(FPA)]
    return pl.pallas_call(
        functools.partial(restrict_kernel, devices, col_count, loads),
        grid=(pairs,),
        in_specs=res_specs + rst_specs + pat_specs,
        out_specs=pl.BlockSpec(memory_space=pl.ANY),
        out_shape=jax.ShapeDtypeStruct((pairs, devices, rows, LANES), jnp.float32),
        scratch_shapes=[
            pltpu.VMEM((3, LANES, LANES), jnp.float32),
            pltpu.VMEM((pairs, devices, rows, LANES), jnp.float32),
            pltpu.SemaphoreType.DMA,
            pltpu.SemaphoreType.DMA,
            pltpu.SemaphoreType.DMA,
        ],
        compiler_params=pltpu.CompilerParams(
            vmem_limit_bytes=VMEM_LIMIT,
            collective_id=1,
            has_side_effects=True,
            dimension_semantics=("arbitrary",),
        ),
        name="restrict_send",
    )(*([residual] * FPA + [restriction] * FPA + [pattern] * FPA))


def gather_kernel(devices, loads, slots_ref, chunk_ref, out_ref, table, ordered):
    pairs = chunk_ref.shape[0]
    few = PAIR * (LANES // devices)
    piece = pairs * few
    lane = lax.broadcasted_iota(jnp.int32, (few, LANES), 1)

    def unpack(f, carry):
        for pair in range(pairs):
            parts = [chunk_ref[pair, f, i * few : (i + 1) * few, :] for i in range(3)]
            for block in range(GROUP):
                moved = []
                for i in range(3):
                    shift = ((i - block) * loads) % LANES
                    moved.append(pltpu.roll(parts[i], shift, 1) if shift else parts[i])
                row = jnp.where(lane < loads, moved[0], jnp.where(lane < 2 * loads, moved[1], moved[2]))
                table[pl.ds(f * (GROUP * piece) + block * piece + pair * few, few), :] = row
        return carry

    lax.fori_loop(0, devices, unpack, 0, unroll=2)
    height = out_ref.shape[0] // (3 * loads)

    def take(r, carry):
        for c in range(LANES):
            ordered[pl.ds(r * LANES + c, 1), :] = table[pl.ds(slots_ref[r * LANES + c], 1), :]
        return carry

    lax.fori_loop(0, height, take, 0)

    def turn(r, carry):
        turned = ordered[pl.ds(pl.multiple_of(r * LANES, LANES), LANES), :].T
        out_ref[pl.ds(r, 3 * loads, stride=height), :] = turned[: 3 * loads, :]
        return carry

    lax.fori_loop(0, height, turn, 0, unroll=4)


def gather(slots, chunks, devices, loads, height):
    return pl.pallas_call(
        functools.partial(gather_kernel, devices, loads),
        in_specs=[pl.BlockSpec(memory_space=pltpu.SMEM), spec_vmem()],
        out_specs=spec_vmem(),
        out_shape=jax.ShapeDtypeStruct((3 * loads * height, LANES), jnp.float32),
        scratch_shapes=[pltpu.VMEM((AGG_DEV, LANES), jnp.float32), pltpu.VMEM((height * LANES, LANES), jnp.float32)],
        compiler_params=pltpu.CompilerParams(vmem_limit_bytes=VMEM_LIMIT),
        name="gather_cells",
    )(slots, chunks)


def scatter_kernel(loads, slots_ref, solution_ref, table, out_ref, ordered):
    height = solution_ref.shape[0] // (3 * loads)

    def turn(r, carry):
        plane = solution_ref[pl.ds(r, 3 * loads, stride=height), :]
        ordered[pl.ds(pl.multiple_of(r * LANES, LANES), LANES), : 3 * loads] = plane.T
        return carry

    lax.fori_loop(0, height, turn, 0, unroll=4)

    def put(r, carry):
        for c in range(LANES):
            table[pl.ds(slots_ref[r * LANES + c], 1), :] = ordered[pl.ds(r * LANES + c, 1), :]
        return carry

    lax.fori_loop(0, height, put, 0)

    def write(q, carry):
        for i in range(3):
            start = pl.multiple_of((i * loads + q) * height, height)
            out_ref[q, i] = solution_ref[pl.ds(start, height), :]
        return carry

    lax.fori_loop(0, loads, write, 0)


def scatter(slots, solution_planes, loads):
    height = solution_planes.shape[0] // (3 * loads)
    return pl.pallas_call(
        functools.partial(scatter_kernel, loads),
        in_specs=[pl.BlockSpec(memory_space=pltpu.SMEM), spec_vmem()],
        out_specs=(spec_vmem(), spec_vmem()),
        out_shape=(
            jax.ShapeDtypeStruct((AGG_DEV, LANES), jnp.float32),
            jax.ShapeDtypeStruct((loads, 3, height, LANES), jnp.float32),
        ),
        scratch_shapes=[pltpu.VMEM((height * LANES, LANES), jnp.float32)],
        compiler_params=pltpu.CompilerParams(vmem_limit_bytes=VMEM_LIMIT),
        name="scatter_cells",
    )(slots, solution_planes)


def pack_kernel(devices, col_count, loads, table, out_ref, sent, send_sem, recv_sem, own_sem):
    piece = AGG_DEV // (GROUP * devices)
    me = lax.axis_index("row") * col_count + lax.axis_index("col")
    barrier = greet(devices, col_count, me)
    lane = lax.broadcasted_iota(jnp.int32, (piece, LANES), 1)

    def pack(f):
        rows = [table[pl.ds(f * (GROUP * piece) + block * piece, piece), :] for block in range(GROUP)]
        for i in range(3):
            total = None
            for block in range(GROUP):
                shift = ((block - i) * loads) % LANES
                moved = pltpu.roll(rows[block], shift, 1) if shift else rows[block]
                total = moved if total is None else jnp.where(lane < block * loads, total, moved)
            sent[f, i * piece : (i + 1) * piece, :] = total

    pack(me)
    own = pltpu.make_async_copy(sent.at[me], out_ref.at[me], own_sem)
    own.start()
    pl.semaphore_wait(barrier, devices - 1)

    def send(index):
        peer, where = peer_of(me, index, devices, col_count)
        pltpu.make_async_remote_copy(
            src_ref=sent.at[peer],
            dst_ref=out_ref.at[me],
            send_sem=send_sem,
            recv_sem=recv_sem,
            device_id=where,
            device_id_type=MESH,
        ).start()

    def step(index, carry):
        pack(peer_of(me, index, devices, col_count)[0])
        send(index - 1)
        return carry

    pack(peer_of(me, 1, devices, col_count)[0])
    lax.fori_loop(2, devices, step, 0)
    send(devices - 1)
    own.wait()
    _, where = peer_of(me, 1, devices, col_count)
    every = pltpu.make_async_remote_copy(
        src_ref=sent.at[pl.ds(0, devices - 1)],
        dst_ref=out_ref.at[pl.ds(0, devices - 1)],
        send_sem=send_sem,
        recv_sem=recv_sem,
        device_id=where,
        device_id_type=MESH,
    )
    every.wait_send()
    every.wait_recv()


def pack_send(table, devices, col_count, loads):
    piece = AGG_DEV // (GROUP * devices)
    return pl.pallas_call(
        functools.partial(pack_kernel, devices, col_count, loads),
        in_specs=[spec_vmem()],
        out_specs=pl.BlockSpec(memory_space=pl.ANY),
        out_shape=jax.ShapeDtypeStruct((devices, 3 * piece, LANES), jnp.float32),
        scratch_shapes=[
            pltpu.VMEM((devices, 3 * piece, LANES), jnp.float32),
            pltpu.SemaphoreType.DMA,
            pltpu.SemaphoreType.DMA,
            pltpu.SemaphoreType.DMA,
        ],
        compiler_params=pltpu.CompilerParams(vmem_limit_bytes=VMEM_LIMIT, collective_id=2, has_side_effects=True),
        name="pack_send",
    )(table)


def sweep_kernel(
    row_count,
    col_count,
    loads,
    rhs_ref,
    inverse_ref,
    blocks_ref,
    pattern_ref,
    planes_ref,
    base,
    x,
    mixed,
    sent,
    halo,
    send_sem,
    recv_sem,
):
    height = inverse_ref.shape[2]
    few = loads // HALVES
    planes = 3 * few
    row = lax.axis_index("row")
    col = lax.axis_index("col")
    exists = (row > 0, row < row_count - 1, col > 0, col < col_count - 1)
    peers = (
        {"row": row - 1, "col": col},
        {"row": row + 1, "col": col},
        {"row": row, "col": col - 1},
        {"row": row, "col": col + 1},
    )
    extent = (planes, planes, height, height)
    barrier = pltpu.get_barrier_semaphore()
    halo[...] = jnp.zeros_like(halo)
    for d in range(4):

        @pl.when(exists[d])
        def _():
            pl.semaphore_signal(barrier, inc=1, device_id=peers[d], device_id_type=MESH)

    lane = lax.broadcasted_iota(jnp.int32, (height, LANES), 1)

    def first(half):
        def one(q, carry):
            source = half * few + q
            for i in range(3):
                total = inverse_ref[i, 0] * rhs_ref[source]
                total = total + inverse_ref[i, 1] * rhs_ref[loads + source]
                total = total + inverse_ref[i, 2] * rhs_ref[2 * loads + source]
                base[half * planes + i * few + q] = total
                x[0, half * planes + i * few + q, 8 : 8 + height, :] = total
            return carry

        lax.fori_loop(0, few, one, 0)

    def pack(slot, step, half):
        own = slice(half * planes, (half + 1) * planes)
        sent[step, half, 0, :planes, :] = x[slot, own, 8, :]
        sent[step, half, 1, :planes, :] = x[slot, own, 7 + height, :]

        def columns(p, carry):
            left, right = carry
            plane = x[slot, half * planes + p, 8 : 8 + height, :]
            left = jnp.where(lane == p, pltpu.roll(plane, p, 1), left)
            right = jnp.where(lane == p, pltpu.roll(plane, p + 1, 1), right)
            return left, right

        blank = jnp.zeros((height, LANES), jnp.float32)
        left, right = lax.fori_loop(0, planes, columns, (blank, blank), unroll=4)
        sent[step, half, 2, :height, :] = left
        sent[step, half, 3, :height, :] = right

    def copy(step, half, d, side):
        return pltpu.make_async_remote_copy(
            src_ref=sent.at[step, half, d, pl.ds(0, extent[d])],
            dst_ref=halo.at[step, half, side, pl.ds(0, extent[d])],
            send_sem=send_sem.at[step, half, d],
            recv_sem=recv_sem.at[step, half, side],
            device_id=peers[d],
            device_id_type=MESH,
        )

    def start(step, half):
        for d in range(4):

            @pl.when(exists[d])
            def _():
                copy(step, half, d, d ^ 1).start()

    def fold(d, carry):
        on = pattern_ref[d].astype(jnp.float32)
        for k in range(3):
            column = [blocks_ref[d, j, k] * on for j in range(3)]
            for i in range(3):
                total = inverse_ref[i, 0] * column[0]
                total = total + inverse_ref[i, 1] * column[1]
                mixed[d, i, k] = total + inverse_ref[i, 2] * column[2]
        return carry

    first(0)
    pack(0, 0, 0)
    present = sum(e.astype(jnp.int32) for e in exists)
    pl.semaphore_wait(barrier, present)
    start(0, 0)
    for half in range(1, HALVES):
        first(half)
        pack(0, 0, half)
        start(0, half)
    lax.fori_loop(0, 4, fold, 0)
    for step in range(ITERS - 1):
        old = step % 2
        last = step == ITERS - 2
        for half in range(HALVES):
            for d in range(4):

                @pl.when(exists[d])
                def _():
                    copy(step, half, d, d).wait_send()
                    copy(step, half, d, d).wait_recv()

            own = slice(half * planes, (half + 1) * planes)
            x[old, own, 7, :] = halo[step, half, 0, :planes, :]
            x[old, own, 8 + height, :] = halo[step, half, 1, :planes, :]

            def update(q, carry):
                totals = [base[half * planes + i * few + q] for i in range(3)]
                for k in range(3):
                    local = k * few + q
                    p = half * planes + local
                    plane = x[old, p, 8 : 8 + height, :]
                    left = jnp.where(
                        lane == 0,
                        pltpu.roll(halo[step, half, 2, :height, :], lax.rem(LANES - local, LANES), 1),
                        pltpu.roll(plane, 1, 1),
                    )
                    right = jnp.where(
                        lane == LANES - 1,
                        pltpu.roll(halo[step, half, 3, :height, :], LANES - 1 - local, 1),
                        pltpu.roll(plane, LANES - 1, 1),
                    )
                    shifted = (x[old, p, 7 : 7 + height, :], x[old, p, 9 : 9 + height, :], left, right)
                    for d in range(4):
                        for i in range(3):
                            totals[i] = totals[i] - mixed[d, i, k] * shifted[d]
                for i in range(3):
                    if last:
                        planes_ref[i * loads + half * few + q] = totals[i]
                    else:
                        x[1 - old, half * planes + i * few + q, 8 : 8 + height, :] = totals[i]
                return carry

            lax.fori_loop(0, few, update, 0)
            if not last:
                pack(1 - old, step + 1, half)
                start(step + 1, half)


def sweeps(rhs, inverse, blocks, pattern, row_count, col_count, loads):
    height = inverse.shape[2]
    planes = 3 * loads
    steps = ITERS - 1
    span = max(planes // HALVES, height)
    return pl.pallas_call(
        functools.partial(sweep_kernel, row_count, col_count, loads),
        in_specs=[spec_vmem()] * 4,
        out_specs=spec_vmem(),
        out_shape=jax.ShapeDtypeStruct((planes, height, LANES), jnp.float32),
        scratch_shapes=[
            pltpu.VMEM((planes, height, LANES), jnp.float32),
            pltpu.VMEM((2, planes, height + 16, LANES), jnp.float32),
            pltpu.VMEM((4, 3, 3, height, LANES), jnp.float32),
            pltpu.VMEM((steps, HALVES, 4, span, LANES), jnp.float32),
            pltpu.VMEM((steps, HALVES, 4, span, LANES), jnp.float32),
            pltpu.SemaphoreType.DMA((steps, HALVES, 4)),
            pltpu.SemaphoreType.DMA((steps, HALVES, 4)),
        ],
        compiler_params=pltpu.CompilerParams(
            vmem_limit_bytes=VMEM_LIMIT, collective_id=0, has_side_effects=True
        ),
        name="sweeps",
    )(rhs.reshape(planes, height, LANES), inverse, blocks, pattern)


def prolong_kernel(devices, loads, chunk_ref, restriction_ref, pattern_ref, out_ref, values):
    groups = AGG_DEV // (LANES * GROUP)
    parts = LANES // devices
    rows = 3 * groups * parts

    @pl.when(pl.program_id(0) == 0)
    def _():
        for i in range(3):
            for group in range(groups):
                start = i * groups * parts + group * parts
                pieces = [chunk_ref[pl.ds(start + part, devices, stride=rows), :] for part in range(parts)]
                values[i, group] = jnp.concatenate(pieces, axis=0).T if parts > 1 else pieces[0].T

    for group in range(groups):
        for block in range(GROUP):
            b = group * GROUP + block
            lanes = slice(b * LANES, (b + 1) * LANES)
            present = pattern_ref[b : b + 1, :].astype(jnp.float32)
            terms = [values[i, group, block * loads : (block + 1) * loads, :] * present for i in range(3)]
            for j in range(3):
                total = restriction_ref[0, j : j + 1, lanes] * terms[0]
                total = total + restriction_ref[1, j : j + 1, lanes] * terms[1]
                out_ref[j, :, lanes] = total + restriction_ref[2, j : j + 1, lanes] * terms[2]


def prolong(chunks, restriction, pattern, devices, loads):
    pattern = pattern.reshape(-1, LANES)
    blocks = AGG_DEV // LANES
    groups = blocks // GROUP
    out = pl.pallas_call(
        functools.partial(prolong_kernel, devices, loads),
        grid=(FPA,),
        in_specs=[
            pl.BlockSpec(chunks.shape, lambda p: (0, 0)),
            pl.BlockSpec((3, 3, AGG_DEV), lambda p: (0, 0, p)),
            pl.BlockSpec((blocks, LANES), lambda p: (p, 0)),
        ],
        out_specs=pl.BlockSpec((3, loads, AGG_DEV), lambda p: (0, 0, p)),
        out_shape=jax.ShapeDtypeStruct((3, loads, restriction.shape[2]), jnp.float32),
        scratch_shapes=[pltpu.VMEM((3, groups, GROUP * loads, LANES), jnp.float32)],
        compiler_params=pltpu.CompilerParams(vmem_limit_bytes=VMEM_LIMIT),
        name="prolong",
    )(chunks, restriction, pattern)
    return out.transpose(1, 0, 2)


def body(
    fine_residual,
    restriction,
    restriction_pattern,
    cell_aggregate,
    block_inverse,
    off_blocks,
    operator_pattern,
):
    loads = fine_residual.shape[0]
    row_count = lax.axis_size("row")
    col_count = lax.axis_size("col")
    devices = row_count * col_count
    height = cell_aggregate.shape[0]
    parts = LANES // devices
    piece = AGG_DEV // (LANES * GROUP) * parts
    owner = cell_aggregate // AGG_DEV
    order = cell_aggregate % AGG_DEV // devices
    cell_block = order // parts
    slots = (
        owner * (GROUP * piece)
        + cell_block % GROUP * piece
        + cell_block // GROUP * parts
        + order % parts
    ).reshape(-1)
    received = restrict(fine_residual, restriction, restriction_pattern, devices, col_count)
    rhs = gather(slots, received, devices, loads, height)
    planes = sweeps(rhs, block_inverse, off_blocks, operator_pattern, row_count, col_count, loads)
    table, iterate = scatter(slots, planes.reshape(-1, LANES), loads)
    arrived = pack_send(table, devices, col_count, loads).reshape(-1, LANES)
    fine_correction = prolong(arrived, restriction, restriction_pattern, devices, loads)
    return (iterate, fine_correction)


def solution(mesh):
    in_specs = (
        P(None, None, ("row", "col")),
        P(None, None, ("row", "col")),
        P(("row", "col")),
        P("row", "col"),
        P(None, None, "row", "col"),
        P(None, None, None, "row", "col"),
        P(None, "row", "col"),
    )
    out_specs = (P(None, None, "row", "col"), P(None, None, ("row", "col")))
    return jax.shard_map(body, mesh=mesh, in_specs=in_specs, out_specs=out_specs, check_vma=False)
```
